256 devices in a mesh: genome: 32 (over z, x_hi, core), samples: 8 (over x_lo, y).
Axes of the slice: x: 4 (x_hi: 2, x_lo: 2; x = x_hi * 2 + x_lo), y: 4, z: 8, core: 2. Of those that a mesh axis runs over, the one named last changes fastest.
Arguments:
- haplotypes: bfloat16 [16384, 32768], P('samples', 'genome'), may hold values from 0 to 1
- window_ends: int32 [32768], P(('genome', 'samples')), may hold values from 1 to 32768, as said below
Outputs:
- ld_score: float32 [32768], P(('genome', 'samples'))
- profile: float32 [2, 32768], P(None, ('genome', 'samples'))
The draws below stay inside these ranges and needn't reach their ends.
Inputs may be any that keep to these rules, and one draw needn't show every extreme that they name: window_ends[v] - v lies between 1 and 1024 for every variant v, and equals 1024 at v = 0.
All inputs are finite; a program needn't handle non-finite values.
Results may differ from the reference program's by a relative error of at most 0.0013.
Values may be sent and summed in bfloat16 or wider, within the bound.
A program may use at most 64 MiB of HBM per device.

```python
import math
import jax
import jax.numpy as jnp
from jax import lax

HAP_DEV = 2048
WIN = 1024
TILE = 128
HAPLOS = 16384
VARIANTS = 32768
SHARE = 128


def smooth_curve(curve_key, row_count, spacing):
    knot_count = VARIANTS // spacing + 3
    knot_key, offset_key = jax.random.split(curve_key)
    knots = jax.random.normal(knot_key, (row_count, knot_count), jnp.float32)
    offsets = jax.random.randint(offset_key, (row_count, 1), 0, spacing)
    placed = jnp.arange(VARIANTS, dtype=jnp.int32)[None, :] + offsets
    left_index = placed // spacing
    fraction = (placed % spacing).astype(jnp.float32) / float(spacing)
    lower = jnp.take_along_axis(knots, left_index, axis=1)
    upper = jnp.take_along_axis(knots, left_index + 1, axis=1)
    return lower * (1.0 - fraction) + upper * fraction


def draw_haplotypes(key, part):
    block_rows = min(HAP_DEV, 256)
    block_total = HAPLOS // block_rows
    threshold = jax.random.uniform(jax.random.fold_in(key, 11), (VARIANTS,), jnp.float32, -1.0, 3.0)
    coarse_space = 4 * WIN
    middle_space = max(WIN // 2, 2)
    fine_space = max(WIN // 16, 2)

    def sample_block(block_index):
        block_key = jax.random.fold_in(jax.random.fold_in(key, 23), block_index)
        sub_keys = jax.random.split(block_key, 4)
        latent = smooth_curve(sub_keys[0], block_rows, coarse_space)
        latent = latent + 0.5 * smooth_curve(sub_keys[1], block_rows, middle_space)
        latent = latent + 0.3 * smooth_curve(sub_keys[2], block_rows, fine_space)
        noise = jax.random.normal(sub_keys[3], (block_rows, VARIANTS), jnp.float32)
        return jax.nn.sigmoid(3.0 * (latent - threshold[None, :]) + noise)
    dosage = lax.map(sample_block, jnp.arange(block_total, dtype=jnp.int32)).reshape(HAPLOS, VARIANTS)
    return dosage.astype(jnp.bfloat16)


def draw_window_ends(key, part):
    spans = jax.random.randint(jax.random.fold_in(key, 37), (VARIANTS,), 1, WIN + 1)
    spans = spans.at[0].set(WIN)
    return jnp.minimum(jnp.arange(VARIANTS, dtype=jnp.int32) + spans, VARIANTS).astype(jnp.int32)


def setup_inputs(seed: int = 0) -> dict:
    key_of = jax.random.split(jax.random.key(seed), 3)
    return {
        "haplotypes": draw_haplotypes(jax.random.fold_in(key_of[2], 71), 0),
        "window_ends": draw_window_ends(jax.random.fold_in(key_of[2], 71), 0),
    }


variance_floor = 0.01

def standardize(alleles, frequency, inverse_sd):
    return ((alleles.astype(jnp.float32) - frequency) * inverse_sd).astype(jnp.bfloat16)

def transpose_product(left_side, right_side):
    return lax.dot_general(left_side, right_side, (((0,), (0,)), ((), ())), preferred_element_type=jnp.float32)

def window_mean(cross_sum, haplo_total, row_position, column_position, window_end):
    correlation = cross_sum / haplo_total
    inside = (column_position > row_position[:, None]) & (column_position < window_end[:, None])
    squares = lax.optimization_barrier(jnp.sum(jnp.where(inside, correlation * correlation, jnp.zeros_like(correlation)), axis=1))
    counted = jnp.maximum(window_end - row_position - 1, 1).astype(jnp.float32)
    return squares / counted

def reference(haplotypes, window_ends):
    haplo_total = float(haplotypes.shape[0])
    variants = haplotypes.shape[1]
    counts = lax.optimization_barrier(jnp.sum(haplotypes, axis=0, dtype=jnp.float32))
    frequency = counts / haplo_total
    inverse_sd = lax.rsqrt(jnp.maximum(frequency * (1.0 - frequency), variance_floor))
    padded_haps = jnp.pad(haplotypes, ((0, 0), (0, WIN)))
    padded_freq = jnp.pad(frequency, (0, WIN))
    padded_isd = jnp.pad(inverse_sd, (0, WIN))

    def tile_scores(tile_index):
        first_row = tile_index * TILE
        columns = lax.dynamic_slice_in_dim(padded_haps, first_row, TILE + WIN, 1)
        standard = standardize(columns, lax.dynamic_slice_in_dim(padded_freq, first_row, TILE + WIN), lax.dynamic_slice_in_dim(padded_isd, first_row, TILE + WIN))
        cross_sum = transpose_product(standard[:, :TILE], standard)
        row_position = first_row + jnp.arange(TILE, dtype=jnp.int32)
        column_position = jnp.broadcast_to(first_row + jnp.arange(TILE + WIN, dtype=jnp.int32)[None, :], (TILE, TILE + WIN))
        window_end = lax.dynamic_slice_in_dim(window_ends, first_row, TILE)
        return window_mean(cross_sum, haplo_total, row_position, column_position, window_end)
    ld_score = lax.map(tile_scores, jnp.arange(variants // TILE, dtype=jnp.int32)).reshape(variants)
    log_rates = jnp.array([math.log(0.5) / (4 * SHARE), math.log(0.1) / variants], jnp.float32)
    decay = jnp.exp(log_rates)

    def advance(state, value):
        state = decay * state + value
        return (state, state)
    _, smoothed = lax.scan(advance, jnp.zeros(2, jnp.float32), ld_score)
    position = jnp.arange(variants, dtype=jnp.float32) + 1.0
    profile = smoothed.T * (-jnp.expm1(log_rates))[:, None] / -jnp.expm1(position[None, :] * log_rates[:, None])
    return (ld_score, profile)
```

```python
import math

import jax
import jax.numpy as jnp
from jax import lax
from jax.experimental import pallas as pl
from jax.experimental.pallas import tpu as pltpu
from jax.sharding import PartitionSpec as P

F32 = jnp.float32
BF16 = jnp.bfloat16
MESH = pl.DeviceIdType.MESH
VARIANCE_FLOOR = 0.01
T = 128
RING = 4


def rate_rows(shape, share, variants):
    row = lax.broadcasted_iota(jnp.int32, shape, 0)
    return jnp.where(row == 0, math.log(0.5) / (4 * share), math.log(0.1) / variants).astype(F32)


def one_minus_exp(x):
    series = jnp.ones_like(x)
    for order in range(9, 1, -1):
        series = 1.0 + series * x * (1.0 / order)
    return jnp.where(x > -0.5, -x * series, 1.0 - jnp.exp(x))


def transposed_dot(a, b):
    return lax.dot_general(a, b, (((0,), (0,)), ((), ())), preferred_element_type=F32)


def kernel_body(
    G, S, x_ref, ends_ref, ld_ref, prof_ref,
    raw, xs, halo, hs, sb, yr, xsend, xrecv, diag, own, score,
    cnt, cnts, tot, htot, stat, hstat, msg1, msgs1, msg2, msgs2, w1, w2,
    load_sem, halo_s, halo_r, cnt_s, cnt_r, stat_s, stat_r,
    y_s, y_r, x_s, x_r, m1_s, m1_r, m2_s, m2_r,
):
    rows = x_ref.shape[0]
    width = x_ref.shape[1]
    C = width // T
    haplos = float(rows * S)
    variants = width * G
    g = lax.axis_index("genome")
    s = lax.axis_index("samples")
    y = lax.rem(s, RING)
    half = s // RING
    partner = lax.rem(s + RING, S)
    before = lax.rem(g + G - 1, G)

    barrier = pltpu.get_barrier_semaphore()

    def greet_s(k, _):
        pl.semaphore_signal(barrier, inc=1, device_id={"samples": lax.rem(s + k, S)}, device_id_type=MESH)
        return 0

    def greet_g(k, _):
        pl.semaphore_signal(barrier, inc=1, device_id={"genome": lax.rem(g + k, G)}, device_id_type=MESH)
        return 0

    def load(c):
        return pltpu.make_async_copy(x_ref.at[:, pl.ds(c * T, T)], raw.at[c], load_sem.at[c])

    for c in range(C):
        load(c).start()
    lax.fori_loop(1, S, greet_s, 0)
    lax.fori_loop(1, G, greet_g, 0)

    ones = jnp.ones((16, rows), BF16)
    for c in range(C):
        load(c).wait()
        sums = jnp.dot(ones, raw[c], preferred_element_type=F32)
        cnt[pl.ds(c, 1), :] = sums[0:1, :]

    pl.semaphore_wait(barrier, S + G - 2)

    def halo_copy(c):
        return pltpu.make_async_remote_copy(
            src_ref=raw.at[c], dst_ref=halo.at[c], send_sem=halo_s.at[c], recv_sem=halo_r.at[c],
            device_id={"genome": before}, device_id_type=MESH,
        )

    def to_samples(src, dst, ss, rs):
        def copy(k):
            return pltpu.make_async_remote_copy(
                src_ref=src, dst_ref=dst.at[s], send_sem=ss.at[k], recv_sem=rs.at[s],
                device_id={"samples": lax.rem(s + k, S)}, device_id_type=MESH,
            )

        def arrival(k):
            peer = lax.rem(s + k, S)
            return pltpu.make_async_remote_copy(
                src_ref=src, dst_ref=dst.at[peer], send_sem=ss.at[k], recv_sem=rs.at[peer],
                device_id={"samples": peer}, device_id_type=MESH,
            )

        return copy, arrival

    cnt_copy, cnt_arrival = to_samples(cnt, cnts, cnt_s, cnt_r)
    for k in range(1, S):
        cnt_copy(k).start()
    for c in range(C):
        halo_copy(c).start()

    rates = rate_rows((8, T), T, variants)

    def weight1(k, _):
        ahead = (s - 1 - k).astype(F32)
        w1[k] = jnp.where(ahead >= 0.0, jnp.exp(jnp.maximum(ahead, 0.0) * T * rates), 0.0)
        return 0

    def weight2(k, _):
        ahead = (g - 1 - k).astype(F32)
        w2[k] = jnp.where(ahead >= 0.0, jnp.exp(jnp.maximum(ahead, 0.0) * width * rates), 0.0)
        return 0

    lax.fori_loop(0, S, weight1, 0)
    lax.fori_loop(0, G, weight2, 0)

    total = cnt[...]
    for k in range(1, S):
        cnt_arrival(k).wait_recv()
    for k in range(1, S):
        total = total + cnts[lax.rem(s + k, S)]
    tot[...] = total
    stat_copy = pltpu.make_async_remote_copy(
        src_ref=tot, dst_ref=htot, send_sem=stat_s, recv_sem=stat_r,
        device_id={"genome": before}, device_id_type=MESH,
    )
    stat_copy.start()

    def statistics(counts, out):
        frequency = counts / haplos
        out[0] = frequency
        out[1] = lax.rsqrt(jnp.maximum(frequency * (1.0 - frequency), VARIANCE_FLOOR))

    statistics(total, stat)

    STEP = 256

    def own_standard(c, _):
        f = stat[0, pl.ds(c, 1), :]
        d = stat[1, pl.ds(c, 1), :]
        for b in range(rows // STEP):
            part = raw[c, pl.ds(b * STEP, STEP), :].astype(F32)
            xs[pl.ds(b * STEP, STEP), pl.ds(pl.multiple_of(c * T, T), T)] = ((part - f) * d).astype(BF16)
        return 0

    lax.fori_loop(0, C, own_standard, 0)

    def y_copy(p, r):
        return pltpu.make_async_remote_copy(
            src_ref=sb.at[r, p], dst_ref=yr.at[y, r // RING, p],
            send_sem=y_s.at[r, p], recv_sem=y_r.at[y, r // RING, p],
            device_id={"samples": half * RING + r % RING}, device_id_type=MESH,
        )

    def y_send(p, r):
        @pl.when(y != r % RING)
        def _():
            y_copy(p, r).start()

    B = 2
    for q in range(C // B):
        product = transposed_dot(xs[:, q * B * T : (q + 1) * B * T], xs[:, : (q + 1) * B * T])
        for p in range(q * B, (q + 1) * B):
            at = (p - q * B) * T
            for r in range(p):
                sb[r, p] = product[at : at + T, r * T : (r + 1) * T].astype(BF16)
            diag[p] = product[at : at + T, p * T : (p + 1) * T]
            for r in range(p):
                y_send(p, r)

    def y_sum(j, p):
        value = sb[j * RING + y, p].astype(F32)
        for k in range(1, RING):
            slot = lax.rem(y + k, RING)
            pltpu.make_async_remote_copy(
                src_ref=sb.at[0, p], dst_ref=yr.at[slot, j, p],
                send_sem=y_s.at[0, p], recv_sem=y_r.at[slot, j, p],
                device_id={"samples": half * RING + slot}, device_id_type=MESH,
            ).wait_recv()
        for k in range(1, RING):
            value = value + yr[lax.rem(y + k, RING), j, p].astype(F32)
        return value

    r_own = half * RING + y
    r_other = (1 - half) * RING + y

    def x_copy(p):
        return pltpu.make_async_remote_copy(
            src_ref=xsend.at[p], dst_ref=xrecv.at[p], send_sem=x_s.at[p], recv_sem=x_r.at[p],
            device_id={"samples": partner}, device_id_type=MESH,
        )

    def other_tile(p, _):
        xsend[p] = y_sum(1 - half, p).astype(BF16)
        x_copy(p).start()
        return 0

    def own_tile(p, _):
        own[p] = y_sum(half, p)
        return 0

    lane = lax.broadcasted_iota(jnp.int32, (T, T), 1)
    sub = lax.broadcasted_iota(jnp.int32, (T, T), 0)

    def finish_tile(p, _):
        x_copy(p).wait_recv()
        value = (own[p] + xrecv[p].astype(F32)) * (1.0 / haplos)
        row = r_own * T + lane
        col = p * T + sub
        end = jnp.broadcast_to(ends_ref[...] - g * width, (T, T))
        inside = ((col > row) & (col < end)) | ((col < row) & (col + width < end))
        score[...] += jnp.sum(jnp.where(inside, value * value, 0.0), axis=0, keepdims=True)
        return 0

    score[...] = jnp.zeros_like(score)

    def halo_chunk(c):
        if c == 0:
            stat_copy.wait_recv()
            statistics(htot[...], hstat)
        halo_copy(c).wait_recv()
        f = hstat[0, c : c + 1, :]
        d = hstat[1, c : c + 1, :]
        for b in range(rows // STEP):
            part = halo[c, pl.ds(b * STEP, STEP), :].astype(F32)
            hs[pl.ds(b * STEP, STEP), :] = ((part - f) * d).astype(BF16)
        product = transposed_dot(hs[...], xs[:, c * T :])
        first = jnp.where(sub > lane, diag[c], product[:, :T])
        sb[c, c] = first.astype(BF16)
        for r in range(c + 1, C):
            sb[r, c] = product[:, (r - c) * T : (r - c + 1) * T].astype(BF16)
        for r in range(c, C):
            y_send(c, r)

    def halo_sums(c):
        @pl.when(r_other >= c)
        def _():
            other_tile(c, 0)

        @pl.when(r_own >= c)
        def _():
            own_tile(c, 0)

    def halo_finish(c):
        @pl.when(r_own >= c)
        def _():
            finish_tile(c, 0)

    SELF_AT = 2
    for c in range(C):
        halo_chunk(c)
        if c == SELF_AT:
            lax.fori_loop(r_other + 1, C, other_tile, 0)
            lax.fori_loop(r_own + 1, C, own_tile, 0)
            for k in range(SELF_AT):
                halo_sums(k)
        elif c > SELF_AT:
            halo_sums(c - 1)
        if c == SELF_AT + 1:
            lax.fori_loop(r_own + 1, C, finish_tile, 0)
            for k in range(SELF_AT):
                halo_finish(k)
        elif c > SELF_AT + 1:
            halo_finish(c - 2)
    halo_sums(C - 1)
    halo_finish(C - 2)
    halo_finish(C - 1)

    row = r_own * T + lax.broadcasted_iota(jnp.int32, (1, T), 1)
    counted = jnp.maximum(ends_ref[...] - g * width - row - 1, 1).astype(F32)
    ld = score[...] / counted
    ld_ref[...] = ld
    step = lax.broadcasted_iota(jnp.int32, (8, T), 1).astype(F32)
    msg1[...] = jnp.broadcast_to(
        jnp.sum(ld * jnp.exp((T - 1.0 - step) * rates), axis=1, keepdims=True), (8, T)
    )
    m1_copy, m1_arrival = to_samples(msg1, msgs1, m1_s, m1_r)
    for k in range(1, S):
        m1_copy(k).start()

    lag = (lane - sub).astype(F32)
    locals_ = []
    for rate in (math.log(0.5) / (4 * T), math.log(0.1) / variants):
        decay = jnp.where(lag >= 0.0, jnp.exp(jnp.maximum(lag, 0.0) * rate), 0.0)
        locals_.append(
            jnp.dot(jnp.broadcast_to(ld, (8, T)), decay, precision=lax.Precision.HIGHEST, preferred_element_type=F32)
        )
    local = jnp.where(lax.broadcasted_iota(jnp.int32, (8, T), 0) == 0, locals_[0], locals_[1])
    place = (g * width + s * T + 1).astype(F32) + step
    norm = one_minus_exp(rates) / one_minus_exp(place * rates)

    for k in range(1, S):
        m1_arrival(k).wait_recv()
    inner = w1[s] * msg1[...]
    whole = msg1[...] * jnp.exp((S - 1 - s).astype(F32) * T * rates)
    for k in range(1, S):
        peer = lax.rem(s + k, S)
        inner = inner + w1[peer] * msgs1[peer]
        whole = whole + msgs1[peer] * jnp.exp((S - 1 - peer).astype(F32) * T * rates)
    msg2[...] = whole

    def m2_copy(k):
        return pltpu.make_async_remote_copy(
            src_ref=msg2, dst_ref=msgs2.at[g], send_sem=m2_s.at[k], recv_sem=m2_r.at[g],
            device_id={"genome": lax.rem(g + k, G)}, device_id_type=MESH,
        )

    def m2_arrival(k):
        peer = lax.rem(g + k, G)
        return pltpu.make_async_remote_copy(
            src_ref=msg2, dst_ref=msgs2.at[peer], send_sem=m2_s.at[k], recv_sem=m2_r.at[peer],
            device_id={"genome": peer}, device_id_type=MESH,
        )

    def m2_start(k, _):
        m2_copy(k).start()
        return 0

    def m2_wait(k, _):
        m2_arrival(k).wait_recv()
        return 0

    lax.fori_loop(1, G, m2_start, 0)

    for c in range(C):
        halo_copy(c).wait_send()
        for r in range(C):
            @pl.when(y != r % RING)
            def _():
                y_copy(c, r).wait_send()
    stat_copy.wait_send()
    lax.fori_loop(0, C, lambda p, _: (x_copy(p).wait_send(), 0)[1], 0)
    for k in range(1, S):
        cnt_copy(k).wait_send()
        m1_copy(k).wait_send()

    lax.fori_loop(1, G, m2_wait, 0)
    outer = jnp.zeros((8, T), F32)
    for k in range(1, G):
        peer = lax.rem(g + k, G)
        outer = outer + w2[peer] * msgs2[peer]
    incoming = inner + outer * jnp.exp((s * T).astype(F32) * rates)
    smoothed = local + incoming * jnp.exp((step + 1.0) * rates)
    prof_ref[...] = (smoothed * norm)[:2]
    lax.fori_loop(1, G, lambda k, _: (m2_copy(k).wait_send(), 0)[1], 0)


def per_device(haplotypes, window_ends):
    G = lax.axis_size("genome")
    S = lax.axis_size("samples")
    rows, width = haplotypes.shape
    C = width // T
    dma = pltpu.SemaphoreType.DMA

    def body(*refs):
        kernel_body(G, S, *refs)

    ld, prof = pl.pallas_call(
        body,
        out_shape=(jax.ShapeDtypeStruct((1, T), F32), jax.ShapeDtypeStruct((2, T), F32)),
        in_specs=[pl.BlockSpec(memory_space=pl.ANY), pl.BlockSpec(memory_space=pltpu.VMEM)],
        out_specs=(pl.BlockSpec(memory_space=pltpu.VMEM), pl.BlockSpec(memory_space=pltpu.VMEM)),
        scratch_shapes=[
            pltpu.VMEM((C, rows, T), BF16),
            pltpu.VMEM((rows, width), BF16),
            pltpu.VMEM((C, rows, T), BF16),
            pltpu.VMEM((rows, T), BF16),
            pltpu.VMEM((C, C, T, T), BF16),
            pltpu.VMEM((RING, 2, C, T, T), BF16),
            pltpu.VMEM((C, T, T), BF16),
            pltpu.VMEM((C, T, T), BF16),
            pltpu.VMEM((C, T, T), F32),
            pltpu.VMEM((C, T, T), F32),
            pltpu.VMEM((1, T), F32),
            pltpu.VMEM((8, T), F32),
            pltpu.VMEM((S, 8, T), F32),
            pltpu.VMEM((8, T), F32),
            pltpu.VMEM((8, T), F32),
            pltpu.VMEM((2, 8, T), F32),
            pltpu.VMEM((2, 8, T), F32),
            pltpu.VMEM((8, T), F32),
            pltpu.VMEM((S, 8, T), F32),
            pltpu.VMEM((8, T), F32),
            pltpu.VMEM((G, 8, T), F32),
            pltpu.VMEM((S, 8, T), F32),
            pltpu.VMEM((G, 8, T), F32),
            dma((C,)), dma((C,)), dma((C,)), dma((S,)), dma((S,)), dma, dma,
            dma((C, C)), dma((RING, 2, C)), dma((C,)), dma((C,)),
            dma((S,)), dma((S,)), dma((G,)), dma((G,)),
        ],
        compiler_params=pltpu.CompilerParams(collective_id=0, has_side_effects=True),
        name="ld_scores",
    )(haplotypes, window_ends.reshape(1, T))
    return ld.reshape(T), prof


def solution(mesh):
    return jax.shard_map(
        per_device,
        mesh=mesh,
        in_specs=(P("samples", "genome"), P(("genome", "samples"))),
        out_specs=(P(("genome", "samples")), P(None, ("genome", "samples"))),
        check_vma=False,
    )
```

```python
import math

import jax
import jax.numpy as jnp
from jax import lax
from jax.experimental import pallas as pl
from jax.experimental.pallas import tpu as pltpu
from jax.sharding import PartitionSpec as P

F32 = jnp.float32
BF16 = jnp.bfloat16
MESH = pl.DeviceIdType.MESH
VARIANCE_FLOOR = 0.01
T = 128
FIRST = 2
AHEAD = 2
RING = 4


def rate_rows(shape, share, variants):
    row = lax.broadcasted_iota(jnp.int32, shape, 0)
    return jnp.where(row == 0, math.log(0.5) / (4 * share), math.log(0.1) / variants).astype(F32)


def one_minus_exp(x):
    series = jnp.ones_like(x)
    for order in range(9, 1, -1):
        series = 1.0 + series * x * (1.0 / order)
    return jnp.where(x > -0.5, -x * series, 1.0 - jnp.exp(x))


def transposed_dot(a, b):
    return lax.dot_general(a, b, (((0,), (0,)), ((), ())), preferred_element_type=F32)


def kernel_body(
    G, S, x_ref, ends_ref, out_ref,
    raw, xs, halo, hs, sb, yr, hb, yh, last, xsend, xrecv, diag, own, score,
    cnt, cnts, tot, htot, stat, hstat, msg1, msgs1, msg2, msgs2, w1, w2,
    load_sem, halo_s, halo_r, cnt_s, cnt_r, stat_s, stat_r,
    y_s, y_r, h_s, h_r, d_s, d_r, x_s, x_r, m1_s, m1_r, m2_s, m2_r,
):
    rows = x_ref.shape[0]
    width = x_ref.shape[1]
    C = width // T
    haplos = float(rows * S)
    variants = width * G
    g = lax.axis_index("genome")
    s = lax.axis_index("samples")
    y = lax.rem(s, RING)
    half = s // RING
    partner = lax.rem(s + RING, S)
    before = lax.rem(g + G - 1, G)

    barrier = pltpu.get_barrier_semaphore()

    def greet_s(k, _):
        pl.semaphore_signal(barrier, inc=1, device_id={"samples": lax.rem(s + k, S)}, device_id_type=MESH)
        return 0

    def greet_g(k, _):
        pl.semaphore_signal(barrier, inc=1, device_id={"genome": lax.rem(g + k, G)}, device_id_type=MESH)
        return 0

    def load(c):
        return pltpu.make_async_copy(x_ref.at[:, pl.ds(c * T, T)], raw.at[c], load_sem.at[c])

    for c in range(C):
        load(c).start()
    lax.fori_loop(1, S, greet_s, 0)
    lax.fori_loop(1, G, greet_g, 0)

    ones = jnp.ones((16, rows), BF16)
    for c in range(C):
        load(c).wait()
        sums = jnp.dot(ones, raw[c], preferred_element_type=F32)
        cnt[pl.ds(c, 1), :] = sums[0:1, :]

    pl.semaphore_wait(barrier, S + G - 2)

    def halo_copy(c):
        return pltpu.make_async_remote_copy(
            src_ref=raw.at[c], dst_ref=halo.at[c], send_sem=halo_s.at[c], recv_sem=halo_r.at[c],
            device_id={"genome": before}, device_id_type=MESH,
        )

    def to_samples(src, dst, ss, rs):
        def copy(k):
            return pltpu.make_async_remote_copy(
                src_ref=src, dst_ref=dst.at[s], send_sem=ss.at[k], recv_sem=rs.at[s],
                device_id={"samples": lax.rem(s + k, S)}, device_id_type=MESH,
            )

        def arrival(k):
            peer = lax.rem(s + k, S)
            return pltpu.make_async_remote_copy(
                src_ref=src, dst_ref=dst.at[peer], send_sem=ss.at[k], recv_sem=rs.at[peer],
                device_id={"samples": peer}, device_id_type=MESH,
            )

        return copy, arrival

    cnt_copy, cnt_arrival = to_samples(cnt, cnts, cnt_s, cnt_r)
    for k in range(1, S):
        cnt_copy(k).start()
    for k in range(1, S):
        cnt_copy(k).wait_send()
    for c in range(FIRST):
        halo_copy(c).start()

    rates = rate_rows((8, T), T, variants)

    def weight1(k, _):
        ahead = (s - 1 - k).astype(F32)
        w1[k] = jnp.where(ahead >= 0.0, jnp.exp(jnp.maximum(ahead, 0.0) * T * rates), 0.0)
        return 0

    def weight2(k, _):
        ahead = (g - 1 - k).astype(F32)
        w2[k] = jnp.where(ahead >= 0.0, jnp.exp(jnp.maximum(ahead, 0.0) * width * rates), 0.0)
        return 0

    lax.fori_loop(0, S, weight1, 0)
    lax.fori_loop(0, G, weight2, 0)

    total = cnt[...]
    for k in range(1, S):
        cnt_arrival(k).wait_recv()
    for k in range(1, S):
        total = total + cnts[lax.rem(s + k, S)]
    tot[...] = total
    stat_copy = pltpu.make_async_remote_copy(
        src_ref=tot, dst_ref=htot, send_sem=stat_s, recv_sem=stat_r,
        device_id={"genome": before}, device_id_type=MESH,
    )
    stat_copy.start()
    for c in range(FIRST, AHEAD):
        halo_copy(c).start()

    def statistics(counts, out):
        frequency = counts / haplos
        out[0] = frequency
        out[1] = lax.rsqrt(jnp.maximum(frequency * (1.0 - frequency), VARIANCE_FLOOR))

    statistics(total, stat)

    STEP = 256

    def own_standard(c, _):
        f = stat[0, pl.ds(c, 1), :]
        d = stat[1, pl.ds(c, 1), :]
        for b in range(rows // STEP):
            part = raw[c, pl.ds(b * STEP, STEP), :].astype(F32)
            xs[pl.ds(b * STEP, STEP), pl.ds(pl.multiple_of(c * T, T), T)] = ((part - f) * d).astype(BF16)
        return 0

    lax.fori_loop(0, C, own_standard, 0)

    def y_copy(r):
        size = C - 1 - r
        return pltpu.make_async_remote_copy(
            src_ref=sb.at[r, pl.ds(r + 1, size)], dst_ref=yr.at[y, r // RING, pl.ds(r + 1, size)],
            send_sem=y_s.at[r], recv_sem=y_r.at[y, r // RING],
            device_id={"samples": half * RING + r % RING}, device_id_type=MESH,
        )

    def y_arrival(slot, r):
        size = C - 1 - r
        return pltpu.make_async_remote_copy(
            src_ref=sb.at[r, pl.ds(r + 1, size)], dst_ref=yr.at[slot, r // RING, pl.ds(r + 1, size)],
            send_sem=y_s.at[r], recv_sem=y_r.at[slot, r // RING],
            device_id={"samples": half * RING + slot}, device_id_type=MESH,
        )

    def h_copy(c, to):
        low = 0 if c <= to else 1
        return pltpu.make_async_remote_copy(
            src_ref=hb.at[c, to, pl.ds(low, 2 - low)], dst_ref=yh.at[y, c, pl.ds(low, 2 - low)],
            send_sem=h_s.at[c, to], recv_sem=h_r.at[y, c],
            device_id={"samples": half * RING + to}, device_id_type=MESH,
        )

    def h_arrival(c, slot, low):
        return pltpu.make_async_remote_copy(
            src_ref=hb.at[c, 0, pl.ds(low, 2 - low)], dst_ref=yh.at[slot, c, pl.ds(low, 2 - low)],
            send_sem=h_s.at[c, 0], recv_sem=h_r.at[slot, c],
            device_id={"samples": half * RING + slot}, device_id_type=MESH,
        )

    def d_copy():
        return pltpu.make_async_remote_copy(
            src_ref=hb.at[C - 1, RING - 1, 1], dst_ref=last.at[s], send_sem=d_s, recv_sem=d_r.at[s],
            device_id={"samples": S - 1}, device_id_type=MESH,
        )

    def d_arrival(k):
        return pltpu.make_async_remote_copy(
            src_ref=hb.at[C - 1, RING - 1, 1], dst_ref=last.at[k], send_sem=d_s, recv_sem=d_r.at[k],
            device_id={"samples": k}, device_id_type=MESH,
        )

    B = 2
    for q in range(C // B):
        product = transposed_dot(xs[:, q * B * T : (q + 1) * B * T], xs[:, : (q + 1) * B * T])
        for p in range(q * B, (q + 1) * B):
            at = (p - q * B) * T
            for r in range(p):
                sb[r, p] = product[at : at + T, r * T : (r + 1) * T].astype(BF16)
            diag[p] = product[at : at + T, p * T : (p + 1) * T]
    for r in range(C - 1):
        @pl.when(y != r % RING)
        def _():
            y_copy(r).start()

    def self_sum(j, p):
        value = sb[j * RING + y, p].astype(F32)
        for k in range(1, RING):
            value = value + yr[lax.rem(y + k, RING), j, p].astype(F32)
        return value

    def halo_sum(j, c):
        value = hb[c, y, j].astype(F32)
        for k in range(1, RING):
            value = value + yh[lax.rem(y + k, RING), c, j].astype(F32)
        return value

    def self_wait(j):
        for r in range(C - 1):
            @pl.when(j * RING + y == r)
            def _():
                for k in range(1, RING):
                    y_arrival(lax.rem(y + k, RING), r).wait_recv()

    def halo_wait(c):
        if c < RING:
            @pl.when(y >= c)
            def _():
                for k in range(1, RING):
                    h_arrival(c, lax.rem(y + k, RING), 0).wait_recv()

        @pl.when((y < c) & (y + RING >= c))
        def _():
            for k in range(1, RING):
                h_arrival(c, lax.rem(y + k, RING), 1).wait_recv()

    r_own = half * RING + y
    r_other = (1 - half) * RING + y

    def x_copy(p):
        return pltpu.make_async_remote_copy(
            src_ref=xsend.at[p], dst_ref=xrecv.at[p], send_sem=x_s.at[p], recv_sem=x_r.at[p],
            device_id={"samples": partner}, device_id_type=MESH,
        )

    def other_tile(p, _):
        xsend[p] = self_sum(1 - half, p).astype(BF16)
        x_copy(p).start()
        return 0

    def own_tile(p, _):
        own[p] = self_sum(half, p)
        return 0

    lane = lax.broadcasted_iota(jnp.int32, (T, T), 1)
    sub = lax.broadcasted_iota(jnp.int32, (T, T), 0)

    def finish_tile(p, _):
        x_copy(p).wait_recv()
        add_squares(p, own[p] + xrecv[p].astype(F32))
        return 0

    def add_squares(p, value):
        value = value * (1.0 / haplos)
        row = r_own * T + lane
        col = p * T + sub
        end = jnp.broadcast_to(ends_ref[...] - g * width, (T, T))
        inside = ((col > row) & (col < end)) | ((col < row) & (col + width < end))
        score[...] += jnp.sum(jnp.where(inside, value * value, 0.0), axis=0, keepdims=True)

    score[...] = jnp.zeros_like(score)

    def halo_chunk(c):
        if c == 0:
            stat_copy.wait_recv()
            statistics(htot[...], hstat)
        halo_copy(c).wait_recv()
        if c + AHEAD < C:
            halo_copy(c).wait_send()
            halo_copy(c + AHEAD).start()
        f = hstat[0, c : c + 1, :]
        d = hstat[1, c : c + 1, :]
        for b in range(rows // STEP):
            part = halo[c, pl.ds(b * STEP, STEP), :].astype(F32)
            hs[pl.ds(b * STEP, STEP), :] = ((part - f) * d).astype(BF16)
        product = transposed_dot(hs[...], xs[:, c * T :])
        first = jnp.where(sub > lane, diag[c], product[:, :T])
        hb[c, c % RING, c // RING] = first.astype(BF16)
        for r in range(c + 1, C):
            hb[c, r % RING, r // RING] = product[:, (r - c) * T : (r - c + 1) * T].astype(BF16)
        if c == C - 1:
            @pl.when(s != S - 1)
            def _():
                d_copy().start()
            return
        for to in range(RING):
            if c <= to + RING:
                @pl.when(y != to)
                def _():
                    h_copy(c, to).start()

    def halo_sums(c):
        halo_wait(c)

        @pl.when(r_other >= c)
        def _():
            xsend[c] = halo_sum(1 - half, c).astype(BF16)
            x_copy(c).start()

        @pl.when(r_own >= c)
        def _():
            own[c] = halo_sum(half, c)

    def halo_finish(c):
        @pl.when(r_own >= c)
        def _():
            finish_tile(c, 0)

    SELF_AT = 3
    for c in range(C):
        halo_chunk(c)
        if c == SELF_AT:
            self_wait(1 - half)
            lax.fori_loop(r_other + 1, C, other_tile, 0)
            self_wait(half)
            lax.fori_loop(r_own + 1, C, own_tile, 0)
            for k in range(SELF_AT):
                halo_sums(k)
        elif c > SELF_AT:
            halo_sums(c - 1)
        if c == SELF_AT + 1:
            lax.fori_loop(r_own + 1, C, finish_tile, 0)
            for k in range(SELF_AT):
                halo_finish(k)
        elif c > SELF_AT + 1:
            halo_finish(c - 2)
    halo_finish(C - 2)

    @pl.when(s == S - 1)
    def _():
        value = hb[C - 1, RING - 1, 1].astype(F32)
        for k in range(S - 1):
            d_arrival(k).wait_recv()
        for k in range(S - 1):
            value = value + last[k].astype(F32)
        add_squares(C - 1, value)

    row = r_own * T + lax.broadcasted_iota(jnp.int32, (1, T), 1)
    counted = jnp.maximum(ends_ref[...] - g * width - row - 1, 1).astype(F32)
    ld = score[...] / counted
    out_ref[0:1] = ld
    step = lax.broadcasted_iota(jnp.int32, (8, T), 1).astype(F32)
    msg1[...] = jnp.broadcast_to(
        jnp.sum(ld * jnp.exp((T - 1.0 - step) * rates), axis=1, keepdims=True), (8, T)
    )
    m1_copy, m1_arrival = to_samples(msg1, msgs1, m1_s, m1_r)
    for k in range(1, S):
        m1_copy(k).start()

    lag = (lane - sub).astype(F32)
    locals_ = []
    for rate in (math.log(0.5) / (4 * T), math.log(0.1) / variants):
        decay = jnp.where(lag >= 0.0, jnp.exp(jnp.maximum(lag, 0.0) * rate), 0.0)
        locals_.append(
            jnp.dot(jnp.broadcast_to(ld, (8, T)), decay, precision=lax.Precision.HIGHEST, preferred_element_type=F32)
        )
    local = jnp.where(lax.broadcasted_iota(jnp.int32, (8, T), 0) == 0, locals_[0], locals_[1])
    place = (g * width + s * T + 1).astype(F32) + step
    norm = one_minus_exp(rates) / one_minus_exp(place * rates)

    for k in range(1, S):
        m1_arrival(k).wait_recv()
    inner = w1[s] * msg1[...]
    whole = msg1[...] * jnp.exp((S - 1 - s).astype(F32) * T * rates)
    for k in range(1, S):
        peer = lax.rem(s + k, S)
        inner = inner + w1[peer] * msgs1[peer]
        whole = whole + msgs1[peer] * jnp.exp((S - 1 - peer).astype(F32) * T * rates)
    msg2[...] = whole

    def m2_copy(k):
        return pltpu.make_async_remote_copy(
            src_ref=msg2, dst_ref=msgs2.at[g], send_sem=m2_s.at[k], recv_sem=m2_r.at[g],
            device_id={"genome": lax.rem(g + k, G)}, device_id_type=MESH,
        )

    def m2_arrival(k):
        peer = lax.rem(g + k, G)
        return pltpu.make_async_remote_copy(
            src_ref=msg2, dst_ref=msgs2.at[peer], send_sem=m2_s.at[k], recv_sem=m2_r.at[peer],
            device_id={"genome": peer}, device_id_type=MESH,
        )

    def m2_start(k, _):
        m2_copy(k).start()
        return 0

    def m2_wait(k, _):
        m2_arrival(k).wait_recv()
        return 0

    lax.fori_loop(1, G, m2_start, 0)

    for c in range(C - AHEAD, C):
        halo_copy(c).wait_send()
    for r in range(C - 1):
        @pl.when(y != r % RING)
        def _():
            y_copy(r).wait_send()
    for to in range(RING):
        @pl.when(y != to)
        def _():
            for c in range(C - 1):
                if c <= to + RING:
                    h_copy(c, to).wait_send()

    @pl.when(s != S - 1)
    def _():
        d_copy().wait_send()

    stat_copy.wait_send()
    for p in range(C):
        @pl.when((r_other < C - 1) | (p < C - 1))
        def _():
            x_copy(p).wait_send()
    for k in range(1, S):
        m1_copy(k).wait_send()

    lax.fori_loop(1, G, m2_wait, 0)
    outer = jnp.zeros((8, T), F32)
    for k in range(1, G):
        peer = lax.rem(g + k, G)
        outer = outer + w2[peer] * msgs2[peer]
    incoming = inner + outer * jnp.exp((s * T).astype(F32) * rates)
    smoothed = local + incoming * jnp.exp((step + 1.0) * rates)
    out_ref[1:3] = (smoothed * norm)[:2]
    lax.fori_loop(1, G, lambda k, _: (m2_copy(k).wait_send(), 0)[1], 0)


def per_device(haplotypes, window_ends):
    G = lax.axis_size("genome")
    S = lax.axis_size("samples")
    rows, width = haplotypes.shape
    C = width // T
    dma = pltpu.SemaphoreType.DMA

    def body(*refs):
        kernel_body(G, S, *refs)

    out = pl.pallas_call(
        body,
        out_shape=jax.ShapeDtypeStruct((8, T), F32),
        in_specs=[pl.BlockSpec(memory_space=pl.ANY), pl.BlockSpec(memory_space=pltpu.VMEM)],
        out_specs=pl.BlockSpec(memory_space=pltpu.VMEM),
        scratch_shapes=[
            pltpu.VMEM((C, rows, T), BF16),
            pltpu.VMEM((rows, width), BF16),
            pltpu.VMEM((C, rows, T), BF16),
            pltpu.VMEM((rows, T), BF16),
            pltpu.VMEM((C, C, T, T), BF16),
            pltpu.VMEM((RING, 2, C, T, T), BF16),
            pltpu.VMEM((C, RING, 2, T, T), BF16),
            pltpu.VMEM((RING, C, 2, T, T), BF16),
            pltpu.VMEM((S, T, T), BF16),
            pltpu.VMEM((C, T, T), BF16),
            pltpu.VMEM((C, T, T), BF16),
            pltpu.VMEM((C, T, T), F32),
            pltpu.VMEM((C, T, T), F32),
            pltpu.VMEM((1, T), F32),
            pltpu.VMEM((8, T), F32),
            pltpu.VMEM((S, 8, T), F32),
            pltpu.VMEM((8, T), F32),
            pltpu.VMEM((8, T), F32),
            pltpu.VMEM((2, 8, T), F32),
            pltpu.VMEM((2, 8, T), F32),
            pltpu.VMEM((8, T), F32),
            pltpu.VMEM((S, 8, T), F32),
            pltpu.VMEM((8, T), F32),
            pltpu.VMEM((G, 8, T), F32),
            pltpu.VMEM((S, 8, T), F32),
            pltpu.VMEM((G, 8, T), F32),
            dma((C,)), dma((C,)), dma((C,)), dma((S,)), dma((S,)), dma, dma,
            dma((C,)), dma((RING, 2)), dma((C, RING)), dma((RING, C)), dma, dma((S,)), dma((C,)), dma((C,)),
            dma((S,)), dma((S,)), dma((G,)), dma((G,)),
        ],
        compiler_params=pltpu.CompilerParams(collective_id=0, has_side_effects=True),
        name="ld_scores",
    )(haplotypes, window_ends.reshape(1, T))
    return out[0], out[1:3]


def solution(mesh):
    return jax.shard_map(
        per_device,
        mesh=mesh,
        in_specs=(P("samples", "genome"), P(("genome", "samples"))),
        out_specs=(P(("genome", "samples")), P(None, ("genome", "samples"))),
        check_vma=False,
    )
```

```python
import math

import jax
import jax.numpy as jnp
from jax import lax
from jax.experimental import pallas as pl
from jax.experimental.pallas import tpu as pltpu
from jax.sharding import PartitionSpec as P

F32 = jnp.float32
BF16 = jnp.bfloat16
MESH = pl.DeviceIdType.MESH
VARIANCE_FLOOR = 0.01
T = 128
FIRST = 2
AHEAD = 2
RING = 4
PLANE = 4


def rate_rows(shape, share, variants):
    row = lax.broadcasted_iota(jnp.int32, shape, 0)
    return jnp.where(row == 0, math.log(0.5) / (4 * share), math.log(0.1) / variants).astype(F32)


def one_minus_exp(x):
    series = jnp.ones_like(x)
    for order in range(9, 1, -1):
        series = 1.0 + series * x * (1.0 / order)
    return jnp.where(x > -0.5, -x * series, 1.0 - jnp.exp(x))


def transposed_dot(a, b):
    return lax.dot_general(a, b, (((0,), (0,)), ((), ())), preferred_element_type=F32)


def kernel_body(
    G, S, x_ref, ends_ref, out_ref,
    raw, xs, halo, hs, sb, yr, hb, yh, last, xsend, xrecv, diag, own, score,
    cnt, cnts, tot, htot, stat, hstat, msg1, msgs1, msg2, msgs2, msg3, msgs3, w1, w2, w3, w4,
    load_sem, halo_s, halo_r, cnt_s, cnt_r, stat_s, stat_r,
    y_s, y_r, h_s, h_r, d_s, d_r, x_s, x_r, m1_s, m1_r, m2_s, m2_r, m3_s, m3_r,
):
    rows = x_ref.shape[0]
    width = x_ref.shape[1]
    C = width // T
    haplos = float(rows * S)
    variants = width * G
    g = lax.axis_index("genome")
    s = lax.axis_index("samples")
    y = lax.rem(s, RING)
    half = s // RING
    partner = lax.rem(s + RING, S)
    before = lax.rem(g + G - 1, G)
    Z = G // PLANE
    z = g // PLANE
    w = lax.rem(g, PLANE)

    barrier = pltpu.get_barrier_semaphore()

    def greet_s(k, _):
        pl.semaphore_signal(barrier, inc=1, device_id={"samples": lax.rem(s + k, S)}, device_id_type=MESH)
        return 0

    def greet_g(to):
        pl.semaphore_signal(barrier, inc=1, device_id={"genome": to}, device_id_type=MESH)

    def load(c):
        return pltpu.make_async_copy(x_ref.at[:, pl.ds(c * T, T)], raw.at[c], load_sem.at[c])

    for c in range(C):
        load(c).start()
    lax.fori_loop(1, S, greet_s, 0)
    greet_g(before)
    greet_g(lax.rem(g + 1, G))
    for k in range(1, PLANE):
        greet_g(z * PLANE + lax.rem(w + k, PLANE))
    for k in range(1, Z):
        greet_g(lax.rem(g + k * PLANE, G))

    ones = jnp.ones((16, rows), BF16)
    for c in range(C):
        load(c).wait()
        sums = jnp.dot(ones, raw[c], preferred_element_type=F32)
        cnt[pl.ds(c, 1), :] = sums[0:1, :]

    pl.semaphore_wait(barrier, S + PLANE + Z - 1)

    def halo_copy(c):
        return pltpu.make_async_remote_copy(
            src_ref=raw.at[c], dst_ref=halo.at[c], send_sem=halo_s.at[c], recv_sem=halo_r.at[c],
            device_id={"genome": before}, device_id_type=MESH,
        )

    def to_samples(src, dst, ss, rs):
        def copy(k):
            return pltpu.make_async_remote_copy(
                src_ref=src, dst_ref=dst.at[s], send_sem=ss.at[k], recv_sem=rs.at[s],
                device_id={"samples": lax.rem(s + k, S)}, device_id_type=MESH,
            )

        def arrival(k):
            peer = lax.rem(s + k, S)
            return pltpu.make_async_remote_copy(
                src_ref=src, dst_ref=dst.at[peer], send_sem=ss.at[k], recv_sem=rs.at[peer],
                device_id={"samples": peer}, device_id_type=MESH,
            )

        return copy, arrival

    cnt_copy, cnt_arrival = to_samples(cnt, cnts, cnt_s, cnt_r)
    for k in range(1, S):
        cnt_copy(k).start()
    for k in range(1, S):
        cnt_copy(k).wait_send()
    for c in range(FIRST):
        halo_copy(c).start()

    rates = rate_rows((8, T), T, variants)

    def decayed(steps):
        ahead = steps.astype(F32)
        return jnp.where(ahead >= 0.0, jnp.exp(jnp.maximum(ahead, 0.0) * rates), 0.0)

    def weight1(k, _):
        w1[k] = decayed((s - 1 - k) * T)
        w4[k] = decayed((S - 1 - k) * T)
        return 0

    def weight2(k, _):
        w2[k] = decayed(jnp.where(k < z, ((z - k) * PLANE - 1 - w) * width, -1))
        return 0

    def weight3(k, _):
        w3[k] = decayed((w - 1 - k) * width)
        return 0

    lax.fori_loop(0, S, weight1, 0)
    lax.fori_loop(0, Z, weight2, 0)
    lax.fori_loop(0, PLANE, weight3, 0)

    total = cnt[...]
    for k in range(1, S):
        cnt_arrival(k).wait_recv()
    for k in range(1, S):
        total = total + cnts[lax.rem(s + k, S)]
    tot[...] = total
    stat_copy = pltpu.make_async_remote_copy(
        src_ref=tot, dst_ref=htot, send_sem=stat_s, recv_sem=stat_r,
        device_id={"genome": before}, device_id_type=MESH,
    )
    stat_copy.start()
    for c in range(FIRST, AHEAD):
        halo_copy(c).start()

    def statistics(counts, out):
        frequency = counts / haplos
        out[0] = frequency
        out[1] = lax.rsqrt(jnp.maximum(frequency * (1.0 - frequency), VARIANCE_FLOOR))

    statistics(total, stat)

    STEP = 256

    def own_standard(c, _):
        f = stat[0, pl.ds(c, 1), :]
        d = stat[1, pl.ds(c, 1), :]
        for b in range(rows // STEP):
            part = raw[c, pl.ds(b * STEP, STEP), :].astype(F32)
            xs[pl.ds(b * STEP, STEP), pl.ds(pl.multiple_of(c * T, T), T)] = ((part - f) * d).astype(BF16)
        return 0

    lax.fori_loop(0, C, own_standard, 0)

    def y_copy(r):
        size = C - 1 - r
        return pltpu.make_async_remote_copy(
            src_ref=sb.at[r, pl.ds(r + 1, size)], dst_ref=yr.at[y, r // RING, pl.ds(r + 1, size)],
            send_sem=y_s.at[r], recv_sem=y_r.at[y, r // RING],
            device_id={"samples": half * RING + r % RING}, device_id_type=MESH,
        )

    def y_arrival(slot, r):
        size = C - 1 - r
        return pltpu.make_async_remote_copy(
            src_ref=sb.at[r, pl.ds(r + 1, size)], dst_ref=yr.at[slot, r // RING, pl.ds(r + 1, size)],
            send_sem=y_s.at[r], recv_sem=y_r.at[slot, r // RING],
            device_id={"samples": half * RING + slot}, device_id_type=MESH,
        )

    def h_copy(c, to):
        low = 0 if c <= to else 1
        return pltpu.make_async_remote_copy(
            src_ref=hb.at[c, to, pl.ds(low, 2 - low)], dst_ref=yh.at[y, c, pl.ds(low, 2 - low)],
            send_sem=h_s.at[c, to], recv_sem=h_r.at[y, c],
            device_id={"samples": half * RING + to}, device_id_type=MESH,
        )

    def h_arrival(c, slot, low):
        return pltpu.make_async_remote_copy(
            src_ref=hb.at[c, 0, pl.ds(low, 2 - low)], dst_ref=yh.at[slot, c, pl.ds(low, 2 - low)],
            send_sem=h_s.at[c, 0], recv_sem=h_r.at[slot, c],
            device_id={"samples": half * RING + slot}, device_id_type=MESH,
        )

    d_copy, d_arrival = to_samples(hb.at[C - 1, RING - 1, 1], last, d_s, d_r)

    B = 2
    for q in range(C // B):
        product = transposed_dot(xs[:, q * B * T : (q + 1) * B * T], xs[:, : (q + 1) * B * T])
        for p in range(q * B, (q + 1) * B):
            at = (p - q * B) * T
            for r in range(p):
                sb[r, p] = product[at : at + T, r * T : (r + 1) * T].astype(BF16)
            diag[p] = product[at : at + T, p * T : (p + 1) * T]
    for r in range(C - 1):
        @pl.when(y != r % RING)
        def _():
            y_copy(r).start()

    def self_sum(j, p):
        value = sb[j * RING + y, p].astype(F32)
        for k in range(1, RING):
            value = value + yr[lax.rem(y + k, RING), j, p].astype(F32)
        return value

    def halo_sum(j, c):
        value = hb[c, y, j].astype(F32)
        for k in range(1, RING):
            value = value + yh[lax.rem(y + k, RING), c, j].astype(F32)
        return value

    def self_wait(j):
        for r in range(C - 1):
            @pl.when(j * RING + y == r)
            def _():
                for k in range(1, RING):
                    y_arrival(lax.rem(y + k, RING), r).wait_recv()

    def halo_wait(c):
        if c < RING:
            @pl.when(y >= c)
            def _():
                for k in range(1, RING):
                    h_arrival(c, lax.rem(y + k, RING), 0).wait_recv()

        @pl.when((y < c) & (y + RING >= c))
        def _():
            for k in range(1, RING):
                h_arrival(c, lax.rem(y + k, RING), 1).wait_recv()

    r_own = half * RING + y
    r_other = (1 - half) * RING + y

    def x_copy(p):
        return pltpu.make_async_remote_copy(
            src_ref=xsend.at[p], dst_ref=xrecv.at[p], send_sem=x_s.at[p], recv_sem=x_r.at[p],
            device_id={"samples": partner}, device_id_type=MESH,
        )

    def other_tile(p, _):
        xsend[p] = self_sum(1 - half, p).astype(BF16)
        x_copy(p).start()
        return 0

    def own_tile(p, _):
        own[p] = self_sum(half, p)
        return 0

    lane = lax.broadcasted_iota(jnp.int32, (T, T), 1)
    sub = lax.broadcasted_iota(jnp.int32, (T, T), 0)

    def finish_tile(p, _):
        x_copy(p).wait_recv()
        add_squares(p, own[p] + xrecv[p].astype(F32))
        return 0

    def add_squares(p, value):
        score[...] += squares(r_own, p, value, ends_ref[...] - g * width)

    def squares(r, p, value, end):
        value = value * (1.0 / haplos)
        row = r * T + lane
        col = p * T + sub
        end = jnp.broadcast_to(end, (T, T))
        inside = ((col > row) & (col < end)) | ((col < row) & (col + width < end))
        return jnp.sum(jnp.where(inside, value * value, 0.0), axis=0, keepdims=True)

    score[...] = jnp.zeros_like(score)

    def halo_chunk(c):
        if c == 0:
            stat_copy.wait_recv()
            statistics(htot[...], hstat)
        halo_copy(c).wait_recv()
        if c + AHEAD < C:
            halo_copy(c).wait_send()
            halo_copy(c + AHEAD).start()
        f = hstat[0, c : c + 1, :]
        d = hstat[1, c : c + 1, :]
        for b in range(rows // STEP):
            part = halo[c, pl.ds(b * STEP, STEP), :].astype(F32)
            hs[pl.ds(b * STEP, STEP), :] = ((part - f) * d).astype(BF16)
        product = transposed_dot(hs[...], xs[:, c * T :])
        first = jnp.where(sub > lane, diag[c], product[:, :T])
        hb[c, c % RING, c // RING] = first.astype(BF16)
        for r in range(c + 1, C):
            hb[c, r % RING, r // RING] = product[:, (r - c) * T : (r - c + 1) * T].astype(BF16)
        if c == C - 1:
            for k in range(1, S):
                d_copy(k).start()
            return
        for to in range(RING):
            if c <= to + RING:
                @pl.when(y != to)
                def _():
                    h_copy(c, to).start()

    def halo_sums(c):
        halo_wait(c)

        @pl.when(r_other >= c)
        def _():
            xsend[c] = halo_sum(1 - half, c).astype(BF16)
            x_copy(c).start()

        @pl.when(r_own >= c)
        def _():
            own[c] = halo_sum(half, c)

    def halo_finish(c):
        @pl.when(r_own >= c)
        def _():
            finish_tile(c, 0)

    SELF_AT = 3
    for c in range(C - 1):
        halo_chunk(c)
        if c == SELF_AT:
            self_wait(1 - half)
            lax.fori_loop(r_other + 1, C, other_tile, 0)
            self_wait(half)
            lax.fori_loop(r_own + 1, C, own_tile, 0)
            for k in range(SELF_AT):
                halo_sums(k)
        elif c > SELF_AT:
            halo_sums(c - 1)
    halo_sums(C - 2)
    lax.fori_loop(r_own + 1, C, finish_tile, 0)
    for c in range(SELF_AT):
        halo_finish(c)
    halo_chunk(C - 1)
    for c in range(SELF_AT, C - 1):
        halo_finish(c)

    step = lax.broadcasted_iota(jnp.int32, (8, T), 1).astype(F32)
    tail = jnp.exp((T - 1.0 - step) * rates)

    def scores(squared, r, end):
        row = r * T + lax.broadcasted_iota(jnp.int32, (1, T), 1)
        return squared / jnp.maximum(end - row - 1, 1).astype(F32)

    def decayed_sum(values):
        return jnp.broadcast_to(jnp.sum(values * tail, axis=1, keepdims=True), (8, T))

    end = ends_ref[...] - g * width
    early = scores(score[...], r_own, end)
    msg1[0] = decayed_sum(early)
    msg1[1] = jnp.broadcast_to(score[...], (8, T))
    msg1[2] = jnp.broadcast_to(end.astype(F32), (8, T))
    m1_copy, m1_arrival = to_samples(msg1, msgs1, m1_s, m1_r)
    for k in range(1, S):
        m1_copy(k).start()
    msgs1[s] = msg1[...]

    value = hb[C - 1, RING - 1, 1].astype(F32)
    for k in range(1, S):
        d_arrival(k).wait_recv()
    for k in range(1, S):
        value = value + last[lax.rem(s + k, S)].astype(F32)
    for k in range(1, S):
        m1_arrival(k).wait_recv()
    last_end = msgs1[S - 1, 2, 0:1, :].astype(jnp.int32)
    last_squared = msgs1[S - 1, 1, 0:1, :] + squares(S - 1, C - 1, value, last_end)
    last_ld = scores(last_squared, S - 1, last_end)
    whole = decayed_sum(last_ld)
    inner = jnp.zeros((8, T), F32)
    for k in range(S - 1):
        inner = inner + w1[k] * msgs1[k, 0]
        whole = whole + w4[k] * msgs1[k, 0]
    msg2[...] = whole

    def to_genome(src, dst, ss, rs, slot, place):
        def copy(k):
            return pltpu.make_async_remote_copy(
                src_ref=src, dst_ref=dst.at[slot(0)], send_sem=ss.at[k], recv_sem=rs.at[slot(0)],
                device_id={"genome": place(k)}, device_id_type=MESH,
            )

        def arrival(k):
            return pltpu.make_async_remote_copy(
                src_ref=src, dst_ref=dst.at[slot(k)], send_sem=ss.at[k], recv_sem=rs.at[slot(k)],
                device_id={"genome": place(k)}, device_id_type=MESH,
            )

        return copy, arrival

    m2_copy, m2_arrival = to_genome(
        msg2, msgs2, m2_s, m2_r, lambda k: lax.rem(z + k, Z), lambda k: lax.rem(g + k * PLANE, G)
    )
    m3_copy, m3_arrival = to_genome(
        msg3, msgs3, m3_s, m3_r, lambda k: lax.rem(w + k, PLANE),
        lambda k: z * PLANE + lax.rem(w + k, PLANE),
    )
    for k in range(1, Z):
        m2_copy(k).start()
    msg3[1] = whole

    ld = jnp.where(s == S - 1, last_ld, early)
    out_ref[0:1] = ld
    lag = (lane - sub).astype(F32)
    locals_ = []
    for rate in (math.log(0.5) / (4 * T), math.log(0.1) / variants):
        decay = jnp.where(lag >= 0.0, jnp.exp(jnp.maximum(lag, 0.0) * rate), 0.0)
        locals_.append(
            jnp.dot(jnp.broadcast_to(ld, (8, T)), decay, precision=lax.Precision.HIGHEST, preferred_element_type=F32)
        )
    local = jnp.where(lax.broadcasted_iota(jnp.int32, (8, T), 0) == 0, locals_[0], locals_[1])
    place = (g * width + s * T + 1).astype(F32) + step
    norm = one_minus_exp(rates) / one_minus_exp(place * rates)

    outer = jnp.zeros((8, T), F32)
    for k in range(1, Z):
        m2_arrival(k).wait_recv()
    for k in range(1, Z):
        peer = lax.rem(z + k, Z)
        outer = outer + w2[peer] * msgs2[peer]
    msg3[0] = outer
    for k in range(1, PLANE):
        m3_copy(k).start()

    for c in range(C - AHEAD, C):
        halo_copy(c).wait_send()
    for r in range(C - 1):
        @pl.when(y != r % RING)
        def _():
            y_copy(r).wait_send()
    for to in range(RING):
        @pl.when(y != to)
        def _():
            for c in range(C - 1):
                if c <= to + RING:
                    h_copy(c, to).wait_send()

    stat_copy.wait_send()
    for p in range(C):
        @pl.when((r_other < C - 1) | (p < C - 1))
        def _():
            x_copy(p).wait_send()
    for k in range(1, S):
        m1_copy(k).wait_send()
        d_copy(k).wait_send()
    for k in range(1, Z):
        m2_copy(k).wait_send()

    for k in range(1, PLANE):
        m3_arrival(k).wait_recv()
    beside = jnp.zeros((8, T), F32)
    for k in range(1, PLANE):
        peer = lax.rem(w + k, PLANE)
        outer = outer + msgs3[peer, 0]
        beside = beside + w3[peer] * msgs3[peer, 1]
    outer = outer * jnp.exp((w * width).astype(F32) * rates) + beside
    incoming = inner + outer * jnp.exp((s * T).astype(F32) * rates)
    smoothed = local + incoming * jnp.exp((step + 1.0) * rates)
    out_ref[1:3] = (smoothed * norm)[:2]
    for k in range(1, PLANE):
        m3_copy(k).wait_send()


def split_rows(all_ref, ld_ref, prof_ref):
    ld_ref[...] = all_ref[0:1]
    prof_ref[...] = all_ref[1:3]


def per_device(haplotypes, window_ends):
    G = lax.axis_size("genome")
    S = lax.axis_size("samples")
    rows, width = haplotypes.shape
    C = width // T
    Z = G // PLANE
    dma = pltpu.SemaphoreType.DMA

    def body(*refs):
        kernel_body(G, S, *refs)

    out = pl.pallas_call(
        body,
        out_shape=jax.ShapeDtypeStruct((8, T), F32),
        in_specs=[pl.BlockSpec(memory_space=pl.ANY), pl.BlockSpec(memory_space=pltpu.VMEM)],
        out_specs=pl.BlockSpec(memory_space=pltpu.VMEM),
        scratch_shapes=[
            pltpu.VMEM((C, rows, T), BF16),
            pltpu.VMEM((rows, width), BF16),
            pltpu.VMEM((C, rows, T), BF16),
            pltpu.VMEM((rows, T), BF16),
            pltpu.VMEM((C, C, T, T), BF16),
            pltpu.VMEM((RING, 2, C, T, T), BF16),
            pltpu.VMEM((C, RING, 2, T, T), BF16),
            pltpu.VMEM((RING, C, 2, T, T), BF16),
            pltpu.VMEM((S, T, T), BF16),
            pltpu.VMEM((C, T, T), BF16),
            pltpu.VMEM((C, T, T), BF16),
            pltpu.VMEM((C, T, T), F32),
            pltpu.VMEM((C, T, T), F32),
            pltpu.VMEM((1, T), F32),
            pltpu.VMEM((8, T), F32),
            pltpu.VMEM((S, 8, T), F32),
            pltpu.VMEM((8, T), F32),
            pltpu.VMEM((8, T), F32),
            pltpu.VMEM((2, 8, T), F32),
            pltpu.VMEM((2, 8, T), F32),
            pltpu.VMEM((3, 8, T), F32),
            pltpu.VMEM((S, 3, 8, T), F32),
            pltpu.VMEM((8, T), F32),
            pltpu.VMEM((Z, 8, T), F32),
            pltpu.VMEM((2, 8, T), F32),
            pltpu.VMEM((PLANE, 2, 8, T), F32),
            pltpu.VMEM((S, 8, T), F32),
            pltpu.VMEM((Z, 8, T), F32),
            pltpu.VMEM((PLANE, 8, T), F32),
            pltpu.VMEM((S, 8, T), F32),
            dma((C,)), dma((C,)), dma((C,)), dma((S,)), dma((S,)), dma, dma,
            dma((C,)), dma((RING, 2)), dma((C, RING)), dma((RING, C)), dma((S,)), dma((S,)), dma((C,)), dma((C,)),
            dma((S,)), dma((S,)), dma((Z,)), dma((Z,)), dma((PLANE,)), dma((PLANE,)),
        ],
        compiler_params=pltpu.CompilerParams(collective_id=0, has_side_effects=True),
        name="ld_scores",
    )(haplotypes, window_ends.reshape(1, T))
    ld, profile = pl.pallas_call(
        split_rows,
        out_shape=(jax.ShapeDtypeStruct((1, T), F32), jax.ShapeDtypeStruct((2, T), F32)),
        name="outputs",
    )(out)
    return ld.reshape(T), profile


def solution(mesh):
    return jax.shard_map(
        per_device,
        mesh=mesh,
        in_specs=(P("samples", "genome"), P(("genome", "samples"))),
        out_specs=(P(("genome", "samples")), P(None, ("genome", "samples"))),
        check_vma=False,
    )
```

```python
import math

import jax
import jax.numpy as jnp
from jax import lax
from jax.experimental import pallas as pl
from jax.experimental.pallas import tpu as pltpu
from jax.sharding import PartitionSpec as P

F32 = jnp.float32
BF16 = jnp.bfloat16
MESH = pl.DeviceIdType.MESH
VARIANCE_FLOOR = 0.01
T = 128
FIRST = 2
AHEAD = 2
RING = 4
PLANE = 4


def rate_rows(shape, share, variants):
    row = lax.broadcasted_iota(jnp.int32, shape, 0)
    return jnp.where(row == 0, math.log(0.5) / (4 * share), math.log(0.1) / variants).astype(F32)


def one_minus_exp(x):
    series = jnp.ones_like(x)
    for order in range(9, 1, -1):
        series = 1.0 + series * x * (1.0 / order)
    return jnp.where(x > -0.5, -x * series, 1.0 - jnp.exp(x))


def transposed_dot(a, b):
    return lax.dot_general(a, b, (((0,), (0,)), ((), ())), preferred_element_type=F32)


def kernel_body(
    G, S, x_ref, ends_ref, out_ref,
    raw, xs, halo, hs, sb, yr, hb, yh, last, xsend, xrecv, xfine, xfiner, diag, own, score,
    cnt, cnts, tot, htot, stat, hstat, msg1, msgs1, msg2, msgs2, msg3, msgs3, w1, w2, w3, w4,
    load_sem, halo_s, halo_r, cnt_s, cnt_r, stat_s, stat_r,
    y_s, y_r, h_s, h_r, d_s, d_r, x_s, x_r, m1_s, m1_r, m2_s, m2_r, m3_s, m3_r,
):
    rows = x_ref.shape[0]
    width = x_ref.shape[1]
    C = width // T
    haplos = float(rows * S)
    variants = width * G
    g = lax.axis_index("genome")
    s = lax.axis_index("samples")
    y = lax.rem(s, RING)
    half = s // RING
    partner = lax.rem(s + RING, S)
    before = lax.rem(g + G - 1, G)
    Z = G // PLANE
    z = g // PLANE
    w = lax.rem(g, PLANE)

    barrier = pltpu.get_barrier_semaphore()

    def greet_s(k, _):
        pl.semaphore_signal(barrier, inc=1, device_id={"samples": lax.rem(s + k, S)}, device_id_type=MESH)
        return 0

    def greet_g(to):
        pl.semaphore_signal(barrier, inc=1, device_id={"genome": to}, device_id_type=MESH)

    def load(c):
        return pltpu.make_async_copy(x_ref.at[:, pl.ds(c * T, T)], raw.at[c], load_sem.at[c])

    for c in range(C):
        load(c).start()
    lax.fori_loop(1, S, greet_s, 0)
    greet_g(before)
    greet_g(lax.rem(g + 1, G))
    for k in range(1, PLANE):
        greet_g(z * PLANE + lax.rem(w + k, PLANE))
    for k in range(1, Z):
        greet_g(lax.rem(g + k * PLANE, G))

    ones = jnp.ones((16, rows), BF16)
    for c in range(C):
        load(c).wait()
        sums = jnp.dot(ones, raw[c], preferred_element_type=F32)
        cnt[pl.ds(c, 1), :] = sums[0:1, :]

    pl.semaphore_wait(barrier, S + PLANE + Z - 1)

    def halo_copy(c):
        return pltpu.make_async_remote_copy(
            src_ref=raw.at[c], dst_ref=halo.at[c], send_sem=halo_s.at[c], recv_sem=halo_r.at[c],
            device_id={"genome": before}, device_id_type=MESH,
        )

    def to_samples(src, dst, ss, rs):
        def copy(k):
            return pltpu.make_async_remote_copy(
                src_ref=src, dst_ref=dst.at[s], send_sem=ss.at[k], recv_sem=rs.at[s],
                device_id={"samples": lax.rem(s + k, S)}, device_id_type=MESH,
            )

        def arrival(k):
            peer = lax.rem(s + k, S)
            return pltpu.make_async_remote_copy(
                src_ref=src, dst_ref=dst.at[peer], send_sem=ss.at[k], recv_sem=rs.at[peer],
                device_id={"samples": peer}, device_id_type=MESH,
            )

        return copy, arrival

    cnt_copy, cnt_arrival = to_samples(cnt, cnts, cnt_s, cnt_r)
    for k in range(1, S):
        cnt_copy(k).start()
    for k in range(1, S):
        cnt_copy(k).wait_send()
    for c in range(FIRST):
        halo_copy(c).start()

    rates = rate_rows((8, T), T, variants)

    def decayed(steps):
        ahead = steps.astype(F32)
        return jnp.where(ahead >= 0.0, jnp.exp(jnp.maximum(ahead, 0.0) * rates), 0.0)

    def weight1(k, _):
        w1[k] = decayed((s - 1 - k) * T)
        w4[k] = decayed((S - 1 - k) * T)
        return 0

    def weight2(k, _):
        w2[k] = decayed(jnp.where(k < z, ((z - k) * PLANE - 1 - w) * width, -1))
        return 0

    def weight3(k, _):
        w3[k] = decayed((w - 1 - k) * width)
        return 0

    lax.fori_loop(0, S, weight1, 0)
    lax.fori_loop(0, Z, weight2, 0)
    lax.fori_loop(0, PLANE, weight3, 0)

    total = cnt[...]
    for k in range(1, S):
        cnt_arrival(k).wait_recv()
    for k in range(1, S):
        total = total + cnts[lax.rem(s + k, S)]
    tot[...] = total
    stat_copy = pltpu.make_async_remote_copy(
        src_ref=tot, dst_ref=htot, send_sem=stat_s, recv_sem=stat_r,
        device_id={"genome": before}, device_id_type=MESH,
    )
    stat_copy.start()
    for c in range(FIRST, AHEAD):
        halo_copy(c).start()

    def statistics(counts, out):
        frequency = counts / haplos
        out[0] = frequency
        out[1] = lax.rsqrt(jnp.maximum(frequency * (1.0 - frequency), VARIANCE_FLOOR))

    statistics(total, stat)

    STEP = 256

    def own_standard(c, _):
        f = stat[0, pl.ds(c, 1), :]
        d = stat[1, pl.ds(c, 1), :]
        for b in range(rows // STEP):
            part = raw[c, pl.ds(b * STEP, STEP), :].astype(F32)
            xs[pl.ds(b * STEP, STEP), pl.ds(pl.multiple_of(c * T, T), T)] = ((part - f) * d).astype(BF16)
        return 0

    lax.fori_loop(0, C, own_standard, 0)

    def y_copy(r):
        size = C - 1 - r
        return pltpu.make_async_remote_copy(
            src_ref=sb.at[r, pl.ds(r + 1, size)], dst_ref=yr.at[y, r // RING, pl.ds(r + 1, size)],
            send_sem=y_s.at[r], recv_sem=y_r.at[y, r // RING],
            device_id={"samples": half * RING + r % RING}, device_id_type=MESH,
        )

    def y_arrival(slot, r):
        size = C - 1 - r
        return pltpu.make_async_remote_copy(
            src_ref=sb.at[r, pl.ds(r + 1, size)], dst_ref=yr.at[slot, r // RING, pl.ds(r + 1, size)],
            send_sem=y_s.at[r], recv_sem=y_r.at[slot, r // RING],
            device_id={"samples": half * RING + slot}, device_id_type=MESH,
        )

    def h_copy(c, to):
        low = 0 if c <= to else 1
        return pltpu.make_async_remote_copy(
            src_ref=hb.at[c, to, pl.ds(low, 2 - low)], dst_ref=yh.at[y, c, pl.ds(low, 2 - low)],
            send_sem=h_s.at[c, to], recv_sem=h_r.at[y, c],
            device_id={"samples": half * RING + to}, device_id_type=MESH,
        )

    def h_arrival(c, slot, low):
        return pltpu.make_async_remote_copy(
            src_ref=hb.at[c, 0, pl.ds(low, 2 - low)], dst_ref=yh.at[slot, c, pl.ds(low, 2 - low)],
            send_sem=h_s.at[c, 0], recv_sem=h_r.at[slot, c],
            device_id={"samples": half * RING + slot}, device_id_type=MESH,
        )

    d_copy, d_arrival = to_samples(hb.at[C - 1, RING - 1, 1], last, d_s, d_r)

    B = 2
    for q in range(C // B):
        product = transposed_dot(xs[:, q * B * T : (q + 1) * B * T], xs[:, : (q + 1) * B * T])
        for p in range(q * B, (q + 1) * B):
            at = (p - q * B) * T
            for r in range(p):
                sb[r, p] = product[at : at + T, r * T : (r + 1) * T].astype(BF16)
            diag[p] = product[at : at + T, p * T : (p + 1) * T]
    for r in range(C - 1):
        @pl.when(y != r % RING)
        def _():
            y_copy(r).start()

    def self_sum(j, p):
        value = sb[j * RING + y, p].astype(F32)
        for k in range(1, RING):
            value = value + yr[lax.rem(y + k, RING), j, p].astype(F32)
        return value

    def halo_sum(j, c, value):
        for k in range(1, RING):
            value = value + yh[lax.rem(y + k, RING), c, j].astype(F32)
        return value

    def self_wait(j):
        for r in range(C - 1):
            @pl.when(j * RING + y == r)
            def _():
                for k in range(1, RING):
                    y_arrival(lax.rem(y + k, RING), r).wait_recv()

    def halo_wait(c):
        if c < RING:
            @pl.when(y >= c)
            def _():
                for k in range(1, RING):
                    h_arrival(c, lax.rem(y + k, RING), 0).wait_recv()

        @pl.when((y < c) & (y + RING >= c))
        def _():
            for k in range(1, RING):
                h_arrival(c, lax.rem(y + k, RING), 1).wait_recv()

    r_own = half * RING + y
    r_other = (1 - half) * RING + y

    def x_copy(p):
        return pltpu.make_async_remote_copy(
            src_ref=xsend.at[p], dst_ref=xrecv.at[p], send_sem=x_s.at[p], recv_sem=x_r.at[p],
            device_id={"samples": partner}, device_id_type=MESH,
        )

    def fine_copy(p):
        return pltpu.make_async_remote_copy(
            src_ref=xfine, dst_ref=xfiner, send_sem=x_s.at[p], recv_sem=x_r.at[p],
            device_id={"samples": partner}, device_id_type=MESH,
        )

    def other_tile(p, _):
        xsend[p] = self_sum(1 - half, p).astype(BF16)
        x_copy(p).start()
        return 0

    def own_tile(p, _):
        own[p] = self_sum(half, p)
        return 0

    lane = lax.broadcasted_iota(jnp.int32, (T, T), 1)
    sub = lax.broadcasted_iota(jnp.int32, (T, T), 0)

    def finish_tile(p, _):
        x_copy(p).wait_recv()
        add_squares(p, own[p] + xrecv[p].astype(F32))
        return 0

    def add_squares(p, value):
        score[...] += squares(r_own, p, value, ends_ref[...] - g * width)

    def squares(r, p, value, end):
        value = value * (1.0 / haplos)
        row = r * T + lane
        col = p * T + sub
        end = jnp.broadcast_to(end, (T, T))
        inside = ((col > row) & (col < end)) | ((col < row) & (col + width < end))
        return jnp.sum(jnp.where(inside, value * value, 0.0), axis=0, keepdims=True)

    score[...] = jnp.zeros_like(score)

    def halo_chunk(c):
        if c == 0:
            stat_copy.wait_recv()
            statistics(htot[...], hstat)
        halo_copy(c).wait_recv()
        if c + AHEAD < C:
            halo_copy(c).wait_send()
            halo_copy(c + AHEAD).start()
        f = hstat[0, c : c + 1, :]
        d = hstat[1, c : c + 1, :]
        for b in range(rows // STEP):
            part = halo[c, pl.ds(b * STEP, STEP), :].astype(F32)
            hs[pl.ds(b * STEP, STEP), :] = ((part - f) * d).astype(BF16)
        product = transposed_dot(hs[...], xs[:, c * T :])
        first = jnp.where(sub > lane, diag[c], product[:, :T])
        diag[c] = first
        hb[c, c % RING, c // RING] = first.astype(BF16)
        for r in range(c + 1, C):
            hb[c, r % RING, r // RING] = product[:, (r - c) * T : (r - c + 1) * T].astype(BF16)
        if c == C - 1:
            for k in range(1, S):
                d_copy(k).start()
            return
        for to in range(RING):
            if c <= to + RING:
                @pl.when(y != to)
                def _():
                    h_copy(c, to).start()

    def halo_sums(c):
        halo_wait(c)

        @pl.when(r_other > c)
        def _():
            xsend[c] = halo_sum(1 - half, c, hb[c, y, 1 - half].astype(F32)).astype(BF16)
            x_copy(c).start()

        @pl.when(r_other == c)
        def _():
            xfine[...] = halo_sum(1 - half, c, diag[c])
            fine_copy(c).start()

        @pl.when(r_own > c)
        def _():
            own[c] = halo_sum(half, c, hb[c, y, half].astype(F32))

        @pl.when(r_own == c)
        def _():
            own[c] = halo_sum(half, c, diag[c])

    def halo_finish(c):
        @pl.when(r_own > c)
        def _():
            finish_tile(c, 0)

        @pl.when(r_own == c)
        def _():
            fine_copy(c).wait_recv()
            add_squares(c, own[c] + xfiner[...])

    SELF_AT = 2
    FINISH_AT = 4
    for c in range(C - 1):
        halo_chunk(c)
        if c == SELF_AT:
            self_wait(1 - half)
            lax.fori_loop(r_other + 1, C, other_tile, 0)
            self_wait(half)
            lax.fori_loop(r_own + 1, C, own_tile, 0)
            for k in range(SELF_AT):
                halo_sums(k)
        elif c > SELF_AT:
            halo_sums(c - 1)
    halo_sums(C - 2)
    lax.fori_loop(r_own + 1, C, finish_tile, 0)
    for c in range(FINISH_AT):
        halo_finish(c)
    halo_chunk(C - 1)
    for c in range(FINISH_AT, C - 1):
        halo_finish(c)

    step = lax.broadcasted_iota(jnp.int32, (8, T), 1).astype(F32)
    tail = jnp.exp((T - 1.0 - step) * rates)

    def scores(squared, r, end):
        row = r * T + lax.broadcasted_iota(jnp.int32, (1, T), 1)
        return squared / jnp.maximum(end - row - 1, 1).astype(F32)

    def decayed_sum(values):
        return jnp.broadcast_to(jnp.sum(values * tail, axis=1, keepdims=True), (8, T))

    end = ends_ref[...] - g * width
    early = scores(score[...], r_own, end)
    msg1[0] = decayed_sum(early)
    msg1[1] = jnp.broadcast_to(score[...], (8, T))
    msg1[2] = jnp.broadcast_to(end.astype(F32), (8, T))
    m1_copy, m1_arrival = to_samples(msg1, msgs1, m1_s, m1_r)
    for k in range(1, S):
        m1_copy(k).start()
    msgs1[s] = msg1[...]

    value = diag[C - 1]
    for k in range(1, S):
        d_arrival(k).wait_recv()
    for k in range(1, S):
        value = value + last[lax.rem(s + k, S)].astype(F32)
    for k in range(1, S):
        m1_arrival(k).wait_recv()
    last_end = msgs1[S - 1, 2, 0:1, :].astype(jnp.int32)
    last_squared = msgs1[S - 1, 1, 0:1, :] + squares(S - 1, C - 1, value, last_end)
    last_ld = scores(last_squared, S - 1, last_end)
    whole = decayed_sum(last_ld)
    inner = jnp.zeros((8, T), F32)
    for k in range(S - 1):
        inner = inner + w1[k] * msgs1[k, 0]
        whole = whole + w4[k] * msgs1[k, 0]
    msg2[...] = whole

    def to_genome(src, dst, ss, rs, slot, place):
        def copy(k):
            return pltpu.make_async_remote_copy(
                src_ref=src, dst_ref=dst.at[slot(0)], send_sem=ss.at[k], recv_sem=rs.at[slot(0)],
                device_id={"genome": place(k)}, device_id_type=MESH,
            )

        def arrival(k):
            return pltpu.make_async_remote_copy(
                src_ref=src, dst_ref=dst.at[slot(k)], send_sem=ss.at[k], recv_sem=rs.at[slot(k)],
                device_id={"genome": place(k)}, device_id_type=MESH,
            )

        return copy, arrival

    m2_copy, m2_arrival = to_genome(
        msg2, msgs2, m2_s, m2_r, lambda k: lax.rem(z + k, Z), lambda k: lax.rem(g + k * PLANE, G)
    )
    m3_copy, m3_arrival = to_genome(
        msg3, msgs3, m3_s, m3_r, lambda k: lax.rem(w + k, PLANE),
        lambda k: z * PLANE + lax.rem(w + k, PLANE),
    )
    for k in range(1, Z):
        m2_copy(k).start()
    msg3[1] = whole

    ld = jnp.where(s == S - 1, last_ld, early)
    out_ref[0:1] = ld
    lag = (lane - sub).astype(F32)
    locals_ = []
    for rate in (math.log(0.5) / (4 * T), math.log(0.1) / variants):
        decay = jnp.where(lag >= 0.0, jnp.exp(jnp.maximum(lag, 0.0) * rate), 0.0)
        locals_.append(
            jnp.dot(jnp.broadcast_to(ld, (8, T)), decay, precision=lax.Precision.HIGHEST, preferred_element_type=F32)
        )
    local = jnp.where(lax.broadcasted_iota(jnp.int32, (8, T), 0) == 0, locals_[0], locals_[1])
    place = (g * width + s * T + 1).astype(F32) + step
    norm = one_minus_exp(rates) / one_minus_exp(place * rates)

    outer = jnp.zeros((8, T), F32)
    for k in range(1, Z):
        m2_arrival(k).wait_recv()
    for k in range(1, Z):
        peer = lax.rem(z + k, Z)
        outer = outer + w2[peer] * msgs2[peer]
    msg3[0] = outer
    for k in range(1, PLANE):
        m3_copy(k).start()

    for c in range(C - AHEAD, C):
        halo_copy(c).wait_send()
    for r in range(C - 1):
        @pl.when(y != r % RING)
        def _():
            y_copy(r).wait_send()
    for to in range(RING):
        @pl.when(y != to)
        def _():
            for c in range(C - 1):
                if c <= to + RING:
                    h_copy(c, to).wait_send()

    stat_copy.wait_send()
    for p in range(C):
        @pl.when(r_other != p)
        def _():
            x_copy(p).wait_send()

        if p < C - 1:
            @pl.when(r_other == p)
            def _():
                fine_copy(p).wait_send()
    for k in range(1, S):
        m1_copy(k).wait_send()
        d_copy(k).wait_send()
    for k in range(1, Z):
        m2_copy(k).wait_send()

    for k in range(1, PLANE):
        m3_arrival(k).wait_recv()
    beside = jnp.zeros((8, T), F32)
    for k in range(1, PLANE):
        peer = lax.rem(w + k, PLANE)
        outer = outer + msgs3[peer, 0]
        beside = beside + w3[peer] * msgs3[peer, 1]
    outer = outer * jnp.exp((w * width).astype(F32) * rates) + beside
    incoming = inner + outer * jnp.exp((s * T).astype(F32) * rates)
    smoothed = local + incoming * jnp.exp((step + 1.0) * rates)
    out_ref[1:3] = (smoothed * norm)[:2]
    for k in range(1, PLANE):
        m3_copy(k).wait_send()


def split_rows(all_ref, ld_ref, prof_ref):
    ld_ref[...] = all_ref[0:1]
    prof_ref[...] = all_ref[1:3]


def per_device(haplotypes, window_ends):
    G = lax.axis_size("genome")
    S = lax.axis_size("samples")
    rows, width = haplotypes.shape
    C = width // T
    Z = G // PLANE
    dma = pltpu.SemaphoreType.DMA

    def body(*refs):
        kernel_body(G, S, *refs)

    out = pl.pallas_call(
        body,
        out_shape=jax.ShapeDtypeStruct((8, T), F32),
        in_specs=[pl.BlockSpec(memory_space=pl.ANY), pl.BlockSpec(memory_space=pltpu.VMEM)],
        out_specs=pl.BlockSpec(memory_space=pltpu.VMEM),
        scratch_shapes=[
            pltpu.VMEM((C, rows, T), BF16),
            pltpu.VMEM((rows, width), BF16),
            pltpu.VMEM((C, rows, T), BF16),
            pltpu.VMEM((rows, T), BF16),
            pltpu.VMEM((C, C, T, T), BF16),
            pltpu.VMEM((RING, 2, C, T, T), BF16),
            pltpu.VMEM((C, RING, 2, T, T), BF16),
            pltpu.VMEM((RING, C, 2, T, T), BF16),
            pltpu.VMEM((S, T, T), BF16),
            pltpu.VMEM((C, T, T), BF16),
            pltpu.VMEM((C, T, T), BF16),
            pltpu.VMEM((T, T), F32),
            pltpu.VMEM((T, T), F32),
            pltpu.VMEM((C, T, T), F32),
            pltpu.VMEM((C, T, T), F32),
            pltpu.VMEM((1, T), F32),
            pltpu.VMEM((8, T), F32),
            pltpu.VMEM((S, 8, T), F32),
            pltpu.VMEM((8, T), F32),
            pltpu.VMEM((8, T), F32),
            pltpu.VMEM((2, 8, T), F32),
            pltpu.VMEM((2, 8, T), F32),
            pltpu.VMEM((3, 8, T), F32),
            pltpu.VMEM((S, 3, 8, T), F32),
            pltpu.VMEM((8, T), F32),
            pltpu.VMEM((Z, 8, T), F32),
            pltpu.VMEM((2, 8, T), F32),
            pltpu.VMEM((PLANE, 2, 8, T), F32),
            pltpu.VMEM((S, 8, T), F32),
            pltpu.VMEM((Z, 8, T), F32),
            pltpu.VMEM((PLANE, 8, T), F32),
            pltpu.VMEM((S, 8, T), F32),
            dma((C,)), dma((C,)), dma((C,)), dma((S,)), dma((S,)), dma, dma,
            dma((C,)), dma((RING, 2)), dma((C, RING)), dma((RING, C)), dma((S,)), dma((S,)), dma((C,)), dma((C,)),
            dma((S,)), dma((S,)), dma((Z,)), dma((Z,)), dma((PLANE,)), dma((PLANE,)),
        ],
        compiler_params=pltpu.CompilerParams(collective_id=0, has_side_effects=True),
        name="ld_scores",
    )(haplotypes, window_ends.reshape(1, T))
    ld, profile = pl.pallas_call(
        split_rows,
        out_shape=(jax.ShapeDtypeStruct((1, T), F32), jax.ShapeDtypeStruct((2, T), F32)),
        name="outputs",
    )(out)
    return ld.reshape(T), profile


def solution(mesh):
    return jax.shard_map(
        per_device,
        mesh=mesh,
        in_specs=(P("samples", "genome"), P(("genome", "samples"))),
        out_specs=(P(("genome", "samples")), P(None, ("genome", "samples"))),
        check_vma=False,
    )
```
